256 devices in a mesh: layer: 4 (over y), row: 8 (over x, z_lo), col: 8 (over z_hi, core).
Axes of the slice: x: 4, y: 4, z: 8 (z_hi: 4, z_lo: 2; z = z_hi * 2 + z_lo), core: 2. Of those that a mesh axis runs over, the one named last changes fastest.
Arguments:
- ancestor: float32 [8192, 8192], P('row', 'col'), may hold values from -768 to 3840, as said below
- coupling: bfloat16 [4, 8192, 1024], P('layer', ('row', 'col')), may hold values from -10 to 10
- fronts: float32 [4, 2, 512, 512], P('layer', None, None, ('row', 'col')), may hold values from -10 to 360, as said below
- tile_pattern: int32 [4, 2, 8], P('layer'), may hold values 0 or 1
Outputs:
- schur: float32 [8192, 8192], P('row', 'col')
- panel_factor: float32 [8192, 512], P(('row', 'col'))
- pivots: float32 [512], P(('row', 'col'))
The draws below stay inside these ranges and needn't reach their ends.
Inputs may be any that keep to these rules, and one draw needn't show every extreme that they name: `ancestor`: symmetric and positive definite; the leading [512, 512] block of schur_0 stays positive definite after all layers' terms are subtracted. `fronts`: each [512, 512] block is symmetric and positive definite, with diagonal entries from 200 to 360 and other entries within -10 to 10.
All inputs are finite; a program needn't handle non-finite values. No bound on the sum of `tile_pattern` on one device may be relied on, other than what follows from the above.
Results may differ from the reference program's by a relative error of at most 0.0008.
Values may be sent and summed in bfloat16 or wider, within the bound.
A program may use at most 128 MiB of HBM per device.

```python
import jax
import jax.numpy as jnp
from jax import lax

S = 8192
TILE = 1024
P_SIZE = 512
NP = 2
ANC = 1
LAYERS = 4
TILES = 8


def draw_ancestor(key, part):
    noise_key, factor_key, diag_key = jax.random.split(jax.random.fold_in(key, 11), 3)
    lowest = (S + LAYERS * NP * P_SIZE) / 8.0
    sample = jnp.clip(jax.random.normal(noise_key, (S, S), jnp.float32), -4.0, 4.0)
    factor = jax.random.normal(factor_key, (S, 2 * P_SIZE), jnp.float32)
    diagonal = jax.random.uniform(diag_key, (S,), jnp.float32, lowest, 1.25 * lowest)
    symmetric = jnp.clip((sample + sample.T) * 0.7071, -4.0, 4.0)
    coupled = jnp.dot(factor, factor.T, precision=lax.Precision.HIGHEST, preferred_element_type=jnp.float32)
    coupled = (coupled + coupled.T) * (0.5 * 0.75 * lowest / (2 * P_SIZE))
    is_diagonal = jnp.eye(S, dtype=bool)
    return jnp.where(is_diagonal, diagonal[:, None] + coupled, symmetric + coupled)


def draw_fronts(key, part):
    first_key, second_key = jax.random.split(jax.random.fold_in(key, 23))
    sample = jnp.clip(jax.random.normal(first_key, (LAYERS, NP, P_SIZE, P_SIZE), jnp.float32), -4.0, 4.0)
    symmetric = 2.5 * jnp.clip((sample + jnp.swapaxes(sample, -1, -2)) * 0.7071, -4.0, 4.0)
    diagonal = jax.random.uniform(second_key, (LAYERS, NP, P_SIZE), jnp.float32, 200.0, 360.0)
    is_diagonal = jnp.eye(P_SIZE, dtype=bool)
    return jnp.where(is_diagonal, diagonal[..., None], symmetric)


def place_ends(array, stream_key, low, largest):
    dims = array.shape
    place = [jax.random.randint(jax.random.fold_in(stream_key, axis), (), 0, dims[axis]) for axis in range(len(dims))]
    array = array.at[tuple(place)].set(low)
    longest = dims.index(max(dims))
    place[longest] = (place[longest] + 1) % dims[longest]
    return array.at[tuple(place)].set(largest)


def level_of(own_key, extent, pieces, least, top_value):
    level = 1.0
    for axis_at, shards_of in pieces:
        draws = jax.random.uniform(jax.random.fold_in(jax.random.fold_in(own_key, 6), axis_at), (shards_of,), jnp.float32, least / len(pieces), top_value / len(pieces))
        level = level * jnp.repeat(jnp.exp(draws), extent[axis_at] // shards_of).reshape((-1,) + (1,) * (len(extent) - 1 - axis_at))
    return level


def bell_draw(key, extent, deviation, limit, cuts=(), kind=jnp.bfloat16):
    drawn = deviation * jax.random.normal(key, extent, jnp.float32)
    if cuts:
        drawn = drawn * level_of(key, extent, cuts, -0.22, 0.18)
    return jnp.clip(drawn, -limit, limit).astype(kind)


def setup_inputs(seed: int = 0) -> dict:
    key_list = jax.random.split(jax.random.key(seed), 5)
    ancestor = draw_ancestor(jax.random.fold_in(key_list[4], 71), 0)
    coupling = bell_draw(key_list[1], (LAYERS, S, NP * P_SIZE), 2.5, 10.0, ((0, 4), (1, 64)))
    fronts = draw_fronts(jax.random.fold_in(key_list[4], 71), 0)
    tile_pattern = place_ends((jax.random.randint(key_list[3], (LAYERS, NP, TILES), 0, 4) < 3).astype(jnp.int32), jax.random.fold_in(key_list[3], 1), 0, 1)
    return dict(ancestor=ancestor, coupling=coupling, fronts=fronts, tile_pattern=tile_pattern)


def reference(ancestor, coupling, fronts, tile_pattern):
    front_chol = jnp.linalg.cholesky(fronts)
    tile_of_row = jnp.arange(S, dtype=jnp.int32) // TILE
    onehot = (tile_of_row[:, None] == jnp.arange(S // TILE, dtype=jnp.int32)[None, :]).astype(jnp.float32)
    schur = ancestor
    for layer_id in range(LAYERS):
        row_masks = jnp.dot(onehot, tile_pattern[layer_id].T.astype(jnp.float32))
        solved_parts = []
        for panel in range(NP):
            columns = coupling[layer_id, :, panel * P_SIZE:(panel + 1) * P_SIZE].astype(jnp.float32) * row_masks[:, panel:panel + 1]
            solved_parts.append(lax.linalg.triangular_solve(front_chol[layer_id, panel], columns, left_side=False, lower=True, transpose_a=True))
        scaled = jnp.concatenate(solved_parts, 1).astype(jnp.bfloat16)
        schur = schur - jnp.dot(scaled.astype(jnp.float32), scaled.T.astype(jnp.float32), preferred_element_type=jnp.float32)
    global_rows = jnp.arange(S, dtype=jnp.int32)
    panels = []
    pivot_list = []
    for section in range(ANC):
        offset = section * P_SIZE
        pivot_chol = jnp.linalg.cholesky(schur[offset:offset + P_SIZE, offset:offset + P_SIZE])
        solved = lax.linalg.triangular_solve(pivot_chol, schur[:, offset:offset + P_SIZE], left_side=False, lower=True, transpose_a=True)
        panel_rows = jnp.where((global_rows >= offset)[:, None], solved, jnp.zeros_like(solved))
        schur = schur - jnp.dot(panel_rows.astype(jnp.float32), panel_rows.T.astype(jnp.float32), precision=lax.Precision.HIGHEST, preferred_element_type=jnp.float32)
        panels.append(panel_rows)
        diagonal = jnp.diagonal(pivot_chol)
        pivot_list.append(diagonal * diagonal)
    return (schur, jnp.concatenate(panels, 1), jnp.concatenate(pivot_list))
```

```python
import functools
import jax, jax.numpy as jnp
from jax import lax
from jax.experimental import pallas as pl
from jax.experimental.pallas import tpu as pltpu
from jax.sharding import PartitionSpec as P

F32, BF16 = jnp.float32, jnp.bfloat16
N, B, SB = 512, 128, 16

def split(a):
    hi = a.astype(BF16)
    return hi, (a - hi.astype(F32)).astype(BF16)

def dot3(a, b, dims=((1,), (0,))):
    ah, al = a
    bh, bl = b
    d = functools.partial(lax.dot_general, dimension_numbers=(dims, ((), ())), preferred_element_type=F32)
    return d(ah, bh) + (d(al, bh) + d(ah, bl))

def factor_block(dts):
    sub = lax.broadcasted_iota(jnp.int32, (SB, B), 0)
    sub2 = lax.broadcasted_iota(jnp.int32, (SB, 2 * B), 0)
    for s in range(B // SB):
        lo = s * SB
        state = []
        for dt in dts:
            rows = dt[lo:lo + SB, :]
            cols = [jnp.broadcast_to(rows[:, lo + j:lo + j + 1], (SB, B)) for j in range(SB)]
            state.append([rows, cols, []])
        for j in range(SB):
            for st in state:
                g, cols, xs = st
                cj = cols[j]
                d = cj[j:j + 1, :]
                rinv = 1.0 / d
                rs = lax.rsqrt(d)
                row = g[j:j + 1, :]
                xs.append(row * jnp.concatenate([rs, rs], 1))
                rowg = row * jnp.concatenate([rinv, rinv], 1)
                cj2 = jnp.concatenate([cj, cj], 1)
                st[0] = jnp.where(sub2 == j, jnp.broadcast_to(rowg, (SB, 2 * B)), g - cj2 * rowg)
                for k in range(j + 1, SB):
                    ck = cols[k]
                    t = ck[j:j + 1, :] * rinv
                    cols[k] = jnp.where(sub == j, jnp.broadcast_to(t, (SB, B)), ck - cj * t)
        for dt, (g, cols, xs) in zip(dts, state):
            if lo + SB < B:
                rest = slice(lo + SB, B)
                pieces = ([jnp.zeros((lo, 2 * B), F32)] if lo else []) + [g, jnp.zeros((B - lo - SB, 2 * B), F32)]
                pad = jnp.concatenate(pieces, 0)
                dt[rest, :] = dt[rest, :] - dot3(split(dt[rest, 0:B]), split(pad))
            dt[lo:lo + SB, :] = jnp.concatenate(xs, 0)

def chol_steps(a_refs, y_refs, dts, xrs):
    n = len(a_refs)
    eye = (lax.broadcasted_iota(jnp.int32, (B, B), 0) == lax.broadcasted_iota(jnp.int32, (B, B), 1)).astype(F32)
    for y in y_refs:
        y[...] = jnp.zeros((N, N), F32)
    for k in range(N // B):
        for y in y_refs:
            y[k * B:(k + 1) * B, k * B:(k + 1) * B] = eye

    def outer(k, _):
        o = pl.multiple_of(k * B, B)
        blk = pl.ds(o, B)
        for a, dt in zip(a_refs, dts):
            dt[:, 0:B] = a[blk, blk]
            dt[:, B:2 * B] = eye
        factor_block(dts)
        for a, y, dt, xr in zip(a_refs, y_refs, dts, xrs):
            t = split(dt[:, B:2 * B])
            xr[:, 0:N] = dot3(t, split(a[blk, :]))
            yk = dot3(t, split(y[blk, :]))
            xr[:, N:2 * N] = yk
            y[blk, :] = yk

        def inner(i, _):
            oi = pl.multiple_of(i * B, B)
            bi = pl.ds(oi, B)
            for a, y, xr in zip(a_refs, y_refs, xrs):
                up = dot3(split(xr[:, bi]), split(xr[...]), ((0,), (0,)))
                a[bi, :] = a[bi, :] - up[:, 0:N]
                y[bi, :] = y[bi, :] - up[:, N:2 * N]
            return 0
        lax.fori_loop(k + 1, N // B, inner, 0)
        return 0
    lax.fori_loop(0, N // B, outer, 0)

def fronts_kernel(g, out_ref, *scr):
    a, y, dt, xr = (scr[i * 2:(i + 1) * 2] for i in range(4))

    def move(r, _):
        for zh in range(4):
            for core in range(2):
                rows = pl.ds(pl.multiple_of(64 * r + 16 * zh + 8 * core, 8), 8)
                for p in range(2):
                    a[p][rows, :] = g[r, zh, core, p].astype(F32)
        return 0

    lax.fori_loop(0, 8, move, 0)
    chol_steps(a, y, dt, xr)
    for p in range(2):
        out_ref[p] = y[p][...].astype(BF16)


def pivot_chol_kernel(x, out_ref, a, dt, xr):
    a[...] = x[...]
    chol_steps([a], [out_ref], [dt], [xr])


def chol_scratch(nb, y=True):
    return (
        [pltpu.VMEM((N, N), F32)] * (nb * (1 + y)) + [pltpu.VMEM((B, 2 * B), F32)] * nb + [pltpu.VMEM((B, 2 * N), F32)] * nb
    )


def chol_call(kernel, x, shape, dtype, scratch, flops):
    vm = pl.BlockSpec(memory_space=pltpu.VMEM)
    return pl.pallas_call(
        kernel,
        out_shape=jax.ShapeDtypeStruct(shape, dtype),
        in_specs=[vm],
        out_specs=vm,
        scratch_shapes=scratch,
        cost_estimate=pl.CostEstimate(flops=flops, bytes_accessed=2_000_000, transcendentals=0),
    )(x)


def chol_fronts(g):
    return chol_call(fronts_kernel, g, (2, N, N), BF16, chol_scratch(2), 400_000_000)


def chol_pivot(x):
    return chol_call(pivot_chol_kernel, x, (N, N), F32, chol_scratch(1, False), 300_000_000)


MESH = pl.DeviceIdType.MESH
VM = pltpu.VMEM


class Place:
    def __init__(self):
        self.l, self.r, self.c = (lax.axis_index(a) for a in ("layer", "row", "col"))
        self.x, self.zl = self.r // 2, self.r % 2
        self.zh, self.core = self.c // 2, self.c % 2
        self.z = 2 * self.zh + self.zl
        self.partner = {"col": 2 * self.zh + 1 - self.core}

    def along_z(self, k):
        z = (self.z + k) % 8
        return {"row": 2 * self.x + z % 2, "col": 2 * (z // 2) + self.core}

    def along_x(self, k):
        return {"row": 2 * ((self.x + k) % 4) + self.zl}


class Copies:
    def __init__(self, send, recv):
        self.send, self.recv, self.used, self.open = send, recv, 0, []

    def new(self, src, dst, device, when=None):
        i = self.used
        self.used += 1
        copy = pltpu.make_async_remote_copy(
            src_ref=src, dst_ref=dst, send_sem=self.send.at[i], recv_sem=self.recv.at[i],
            device_id=device, device_id_type=MESH,
        )
        if when is None:
            copy.start()
        else:
            pl.when(when)(copy.start)
        self.open.append((copy, when))
        return copy

    def drain(self):
        for copy, when in self.open:
            if when is None:
                copy.wait_send()
            else:
                pl.when(when)(copy.wait_send)


class Spread64:
    def __init__(self, at, copies, buf):
        self.at, self.copies, self.buf = at, copies, buf

    def first(self, src):
        at = self.at
        slot = self.buf.at[at.r, at.zh, at.core]
        self.a = [self.copies.new(src, slot, at.along_z(k)) for k in range(1, 8)]

    def second(self):
        at = self.at
        for copy in self.a:
            copy.wait_recv()
        part = self.buf.at[pl.ds(2 * at.x, 2), :, at.core]
        self.b = [self.copies.new(part, part, at.along_x(k)) for k in range(1, 4)]

    def third(self):
        for copy in self.b:
            copy.wait_recv()
        part = self.buf.at[:, :, self.at.core]
        self.d = self.copies.new(part, part, self.at.partner)

    def last(self):
        self.d.wait_recv()


class Blocks:
    def __init__(self, at, copies, rows, cols):
        self.at, self.copies, self.rows, self.cols = at, copies, rows, cols

    def first(self, src):
        at, new = self.at, self.copies.new
        self.off = at.r != at.c
        self.perm = new(src, self.cols.at[at.c], {"row": at.c, "col": at.r}, self.off)
        mine = self.rows.at[at.c]
        self.own = new(src, mine, at.partner)
        self.b = [new(src, mine, {"col": 2 * ((at.zh + k) % 4) + at.core}) for k in range(1, 4)]

    def second(self):
        at, new = self.at, self.copies.new
        pl.when(self.off)(self.perm.wait_recv)
        mine = self.cols.at[at.r]
        self.zl = new(mine, mine, {"row": 2 * at.x + 1 - at.zl})
        self.xo = [new(mine, mine, at.along_x(k)) for k in range(1, 4)]

    def third(self):
        at, new = self.at, self.copies.new
        self.zl.wait_recv()
        other = self.cols.at[2 * at.x + 1 - at.zl]
        self.xp = [new(other, other, at.along_x(k)) for k in range(1, 4)]

    def fourth(self):
        at, new = self.at, self.copies.new
        self.fwd = []
        for k in range(1, 4):
            self.b[k - 1].wait_recv()
            slot = self.rows.at[2 * ((at.zh + 4 - k) % 4) + at.core]
            self.fwd.append(new(slot, slot, at.partner))

    def last(self):
        for copy in [self.own, *self.xo, *self.xp, *self.fwd]:
            copy.wait_recv()


def scatter16(at, piece, buf, send, recv):
    source = (at.r == 0) & (at.c < 4)

    def copy(i):
        row, col = 2 * at.c + i // 8, i % 8
        return pltpu.make_async_remote_copy(
            src_ref=piece(i), dst_ref=buf.at[row, col // 2, col % 2], send_sem=send.at[i], recv_sem=recv.at[0],
            device_id={"row": row, "col": col}, device_id_type=MESH,
        )

    def to_all(act):
        def step(i, _):
            pl.when((at.c > 0) | (i > 0))(lambda: act(copy(i)))
            return 0

        lax.fori_loop(0, 16, step, 0)

    start = lambda: to_all(lambda one: one.start())
    done = lambda: to_all(lambda one: one.wait_send())
    pl.when(source)(start)
    is_zero = (at.r == 0) & (at.c == 0)

    def arrived():
        slot = buf.at[at.r, at.zh, at.core]
        pl.when(jnp.logical_not(is_zero))(
            pltpu.make_async_remote_copy(
                src_ref=slot, dst_ref=slot, send_sem=send.at[0], recv_sem=recv.at[0],
                device_id=at.partner, device_id_type=MESH,
            ).wait_recv
        )

    return arrived, lambda: pl.when(source)(done)


def inputs_kernel(fr, m, m16, anc, g, mr, mc, g0, own_a, send, recv, s16, r16, sa, ra, la):
    at = Place()
    copies = Copies(send, recv)
    fronts, lead, blocks = Spread64(at, copies, g), Spread64(at, copies, g0), Blocks(at, copies, mr, mc)
    here = at.zh == at.l

    def handed(e):
        rows = pl.ds(pl.multiple_of(256 * at.l + 128 * e, 128), 128)
        return pltpu.make_async_remote_copy(
            src_ref=anc.at[rows, pl.ds(0, 512)], dst_ref=own_a, send_sem=sa.at[e], recv_sem=ra.at[0],
            device_id={"col": 2 * at.l + e}, device_id_type=MESH,
        )

    def kept():
        return pltpu.make_async_copy(anc.at[pl.ds(0, 128), pl.ds(0, 512)], own_a, la)

    fronts.first(fr)
    arrived, scattered = scatter16(at, lambda i: m16.at[i], g0, s16, r16)
    blocks.first(m)
    corner = (at.c == 0) & (at.l == 0)
    pl.when((at.c == 0) & (at.l > 0))(handed(0).start)
    pl.when(at.c == 0)(handed(1).start)
    pl.when(corner)(lambda: kept().start())
    g[at.r, at.zh, at.core] = fr[...]
    mr[at.c] = m[...]

    @pl.when(at.r == at.c)
    def _():
        mc[at.r] = m[...]

    @pl.when((at.r == 0) & (at.c == 0))
    def _():
        g0[0, 0, 0] = m16[0]

    fronts.second()
    blocks.second()
    arrived()
    lead.first(g0.at[at.r, at.zh, at.core])
    fronts.third()
    blocks.third()
    lead.second()

    def over_y(k):
        return pltpu.make_async_remote_copy(
            src_ref=own_a, dst_ref=own_a, send_sem=sa.at[1 + k], recv_sem=ra.at[1],
            device_id={"layer": (at.l + k) % 4}, device_id_type=MESH,
        )

    pl.when(corner)(lambda: kept().wait())
    pl.when(here & jnp.logical_not(corner))(handed(0).wait_recv)

    @pl.when(here)
    def _():
        for k in range(1, 4):
            over_y(k).start()

    blocks.fourth()
    lead.third()
    fronts.last()
    blocks.last()
    lead.last()
    pl.when(jnp.logical_not(here))(over_y(1).wait_recv)

    @pl.when(here)
    def _():
        for k in range(1, 4):
            over_y(k).wait_send()

    pl.when((at.c == 0) & (at.l > 0))(handed(0).wait_send)
    pl.when(at.c == 0)(handed(1).wait_send)
    copies.drain()
    scattered()


def sems(n):
    return pltpu.SemaphoreType.DMA((n,))


def gather_inputs(fr, m, anc):
    s = jax.ShapeDtypeStruct
    vm = pl.BlockSpec(memory_space=VM)
    return pl.pallas_call(
        inputs_kernel,
        out_shape=[
            s((8, 4, 2, 2, 8, 512), BF16), s((8, 128, 1024), BF16), s((8, 128, 1024), BF16),
            s((8, 4, 2, 8, 1024), BF16), s((128, 512), F32),
        ],
        in_specs=[vm, vm, vm, pl.BlockSpec(memory_space=pl.ANY)],
        out_specs=[vm] * 5,
        scratch_shapes=[sems(40), sems(40), sems(16), sems(1), sems(5), sems(2), pltpu.SemaphoreType.DMA],
        compiler_params=pltpu.CompilerParams(has_side_effects=True),
    )(fr, m, m.reshape(16, 8, 1024), anc)


def pivot_kernel(q, own_a, lead, gp, cr, cc, parts, send, recv, s16, r16, sy, ry):
    at = Place()
    copies = Copies(send, recv)
    ys = []
    for k in range(1, 4):
        ys.append(pltpu.make_async_remote_copy(
            src_ref=q, dst_ref=parts.at[at.l], send_sem=sy.at[k - 1], recv_sem=ry.at[k - 1],
            device_id={"layer": (at.l + k) % 4}, device_id_type=MESH,
        ))
        ys[-1].start()
    parts[at.l] = q[...]
    for copy in ys:
        copy.wait_recv()
    lead[...] = own_a[...] - (((parts[0] + parts[1]) + parts[2]) + parts[3])
    spread, blocks = Spread64(at, copies, gp), Blocks(at, copies, cr, cc)
    arrived, scattered = scatter16(at, lambda i: lead.at[pl.ds(pl.multiple_of(8 * i, 8), 8)], gp, s16, r16)
    cr[at.c] = lead[...]

    @pl.when(at.r == at.c)
    def _():
        cc[at.r] = lead[...]

    @pl.when((at.r == 0) & (at.c == 0))
    def _():
        gp[0, 0, 0] = lead[0:8, :]

    arrived()
    spread.first(gp.at[at.r, at.zh, at.core])
    blocks.first(lead)
    spread.second()
    blocks.second()
    spread.third()
    blocks.third()
    blocks.fourth()
    spread.last()
    blocks.last()
    copies.drain()
    scattered()
    for copy in ys:
        copy.wait_send()


def gather_pivot(q, own_a):
    s = jax.ShapeDtypeStruct
    vm = pl.BlockSpec(memory_space=VM)
    return pl.pallas_call(
        pivot_kernel,
        out_shape=[s((128, 512), F32), s((8, 4, 2, 8, 512), F32), s((8, 128, 512), F32), s((8, 128, 512), F32)],
        in_specs=[vm, vm],
        out_specs=[vm] * 4,
        scratch_shapes=[pltpu.VMEM((4, 128, 512), F32), sems(30), sems(30), sems(16), sems(1), sems(3), sems(3)],
        compiler_params=pltpu.CompilerParams(has_side_effects=True),
        cost_estimate=pl.CostEstimate(flops=200_000_000, bytes_accessed=8_000_000, transcendentals=0),
    )(q, own_a)


def local(ancestor, coupling, fronts, tile_pattern):
    r, c = lax.axis_index("row"), lax.axis_index("col")
    fr = jnp.swapaxes(fronts[0], 1, 2).astype(BF16)
    on = lax.dynamic_slice_in_dim(tile_pattern[0], r, 1, 1)
    masked = coupling[0] * jnp.repeat(on[:, 0], 512)[None, :].astype(BF16)
    g, mr, mc, m0, own_a = gather_inputs(fr, masked, ancestor)
    inv = chol_fronts(g)

    def solved(rows):
        out = [
            lax.dot_general(rows[:, p * 512:(p + 1) * 512], inv[p], (((1,), (1,)), ((), ())), preferred_element_type=F32)
            for p in range(2)
        ]
        return jnp.concatenate(out, 1).astype(BF16)

    outer = lambda a, b: lax.dot_general(a, b, (((1,), (1,)), ((), ())), preferred_element_type=F32)
    q = outer(solved(masked), solved(m0.reshape(512, 1024)))
    row_side, col_side = solved(mr.reshape(1024, 1024)), solved(mc.reshape(1024, 1024))
    update = outer(row_side, col_side).astype(BF16)
    share = lax.psum_scatter(update, "layer", scatter_dimension=0, tiled=True)
    summed = lax.all_gather(share, "layer", axis=0, tiled=True)
    lead, gp, cr, cc = gather_pivot(q, own_a)
    pinv = chol_pivot(gp.reshape(512, 512))
    high = functools.partial(
        lax.dot_general, dimension_numbers=(((1,), (1,)), ((), ())), precision=lax.Precision.HIGH, preferred_element_type=F32
    )
    rows = high(cr.reshape(1024, 512), pinv)
    cols = high(cc.reshape(1024, 512), pinv)
    schur = ancestor - summed.astype(F32) - high(rows, cols)
    panel = high(lead, pinv)
    scale = jnp.diagonal(lax.dynamic_slice(pinv, (8 * (8 * r + c), 0), (8, 512)).reshape(8, 64, 8)[:, 8 * r + c])
    return schur, panel, 1.0 / (scale * scale)


def solution(mesh):
    return jax.shard_map(
        local,
        mesh=mesh,
        in_specs=(
            P("row", "col"),
            P("layer", ("row", "col"), None),
            P("layer", None, None, ("row", "col")),
            P("layer", None, None),
        ),
        out_specs=(P("row", "col"), P(("row", "col"), None), P(("row", "col"))),
        check_vma=False,
    )
```

```python
import functools
import jax, jax.numpy as jnp
from jax import lax
from jax.experimental import pallas as pl
from jax.experimental.pallas import tpu as pltpu
from jax.sharding import PartitionSpec as P

F32, BF16 = jnp.float32, jnp.bfloat16
N, B, SB = 512, 128, 16

def split(a):
    hi = a.astype(BF16)
    return hi, (a - hi.astype(F32)).astype(BF16)

def dot3(a, b, dims=((1,), (0,))):
    ah, al = a
    bh, bl = b
    d = functools.partial(lax.dot_general, dimension_numbers=(dims, ((), ())), preferred_element_type=F32)
    return d(ah, bh) + (d(al, bh) + d(ah, bl))

def factor_block(dts):
    sub = lax.broadcasted_iota(jnp.int32, (SB, B), 0)
    sub2 = lax.broadcasted_iota(jnp.int32, (SB, 2 * B), 0)
    for s in range(B // SB):
        lo = s * SB
        state = []
        for dt in dts:
            rows = dt[lo:lo + SB, :]
            cols = [jnp.broadcast_to(rows[:, lo + j:lo + j + 1], (SB, B)) for j in range(SB)]
            state.append([rows, cols, []])
        for j in range(SB):
            for st in state:
                g, cols, xs = st
                cj = cols[j]
                d = cj[j:j + 1, :]
                rinv = 1.0 / d
                rs = lax.rsqrt(d)
                row = g[j:j + 1, :]
                xs.append(row * jnp.concatenate([rs, rs], 1))
                rowg = row * jnp.concatenate([rinv, rinv], 1)
                cj2 = jnp.concatenate([cj, cj], 1)
                st[0] = jnp.where(sub2 == j, jnp.broadcast_to(rowg, (SB, 2 * B)), g - cj2 * rowg)
                for k in range(j + 1, SB):
                    ck = cols[k]
                    t = ck[j:j + 1, :] * rinv
                    cols[k] = jnp.where(sub == j, jnp.broadcast_to(t, (SB, B)), ck - cj * t)
        for dt, (g, cols, xs) in zip(dts, state):
            if lo + SB < B:
                rest = slice(lo + SB, B)
                pieces = ([jnp.zeros((lo, 2 * B), F32)] if lo else []) + [g, jnp.zeros((B - lo - SB, 2 * B), F32)]
                pad = jnp.concatenate(pieces, 0)
                dt[rest, :] = dt[rest, :] - dot3(split(dt[rest, 0:B]), split(pad))
            dt[lo:lo + SB, :] = jnp.concatenate(xs, 0)

def chol_steps(a_refs, y_refs, dts, xrs, stages=()):
    n = len(a_refs)
    eye = (lax.broadcasted_iota(jnp.int32, (B, B), 0) == lax.broadcasted_iota(jnp.int32, (B, B), 1)).astype(F32)
    for y in y_refs:
        y[...] = jnp.zeros((N, N), F32)
    for k in range(N // B):
        for y in y_refs:
            y[k * B:(k + 1) * B, k * B:(k + 1) * B] = eye

    def outer(k, _):
        o = pl.multiple_of(k * B, B)
        blk = pl.ds(o, B)
        for a, dt in zip(a_refs, dts):
            dt[:, 0:B] = a[blk, blk]
            dt[:, B:2 * B] = eye
        factor_block(dts)
        for a, y, dt, xr in zip(a_refs, y_refs, dts, xrs):
            t = split(dt[:, B:2 * B])
            xr[:, 0:N] = dot3(t, split(a[blk, :]))
            yk = dot3(t, split(y[blk, :]))
            xr[:, N:2 * N] = yk
            y[blk, :] = yk

        def inner(i, _):
            oi = pl.multiple_of(i * B, B)
            bi = pl.ds(oi, B)
            for a, y, xr in zip(a_refs, y_refs, xrs):
                up = dot3(split(xr[:, bi]), split(xr[...]), ((0,), (0,)))
                a[bi, :] = a[bi, :] - up[:, 0:N]
                y[bi, :] = y[bi, :] - up[:, N:2 * N]
            return 0
        lax.fori_loop(k + 1, N // B, inner, 0)
        for i, stage in enumerate(stages):
            pl.when(k == i)(stage)
        return 0
    lax.fori_loop(0, N // B, outer, 0)

def chol_scratch(nb, y=True):
    return (
        [pltpu.VMEM((N, N), F32)] * (nb * (1 + y)) + [pltpu.VMEM((B, 2 * B), F32)] * nb + [pltpu.VMEM((B, 2 * N), F32)] * nb
    )


MESH = pl.DeviceIdType.MESH
VM = pltpu.VMEM
WHOLE, LOW, HIGH = pl.ds(0, 128), pl.ds(0, 64), pl.ds(64, 64)


class Place:
    def __init__(self):
        self.l, self.r, self.c = (lax.axis_index(a) for a in ("layer", "row", "col"))
        self.x, self.zl = self.r // 2, self.r % 2
        self.zh, self.core = self.c // 2, self.c % 2
        self.z = 2 * self.zh + self.zl
        self.d = 8 * self.r + self.c
        self.partner = {"col": 2 * self.zh + 1 - self.core}
        self.mirror = {"row": self.c, "col": self.r}
        self.off = self.r != self.c

    def along_z(self, k):
        z = (self.z + k) % 8
        return {"row": 2 * self.x + z % 2, "col": 2 * (z // 2) + self.core}

    def along_x(self, k):
        return {"row": 2 * ((self.x + k) % 4) + self.zl}

    def along_y(self, k):
        return {"layer": (self.l + k) % 4}


class Copies:
    def __init__(self, send, recv):
        self.send, self.recv, self.all = send, recv, []

    def new(self, src, dst, device, when=None):
        i = len(self.all)
        self.all.append((pltpu.make_async_remote_copy(
            src_ref=src, dst_ref=dst, send_sem=self.send.at[i], recv_sem=self.recv.at[i],
            device_id=device, device_id_type=MESH,
        ), when))
        return self.all[-1]

    def drain(self):
        for copy, when in self.all:
            act(when, copy.wait_send)


def act(when, f):
    if when is None:
        f()
    else:
        pl.when(when)(f)


def start(*copies):
    for copy, when in copies:
        act(when, copy.start)


def arrive(*copies):
    for copy, when in copies:
        act(when, copy.wait_recv)


def meet(at, extra=()):
    barrier = pltpu.get_barrier_semaphore()

    def greet(device):
        pl.semaphore_signal(barrier, inc=1, device_id=device, device_id_type=MESH)

    for k in range(1, 8):
        greet(at.along_z(k))
    for k in range(1, 4):
        greet(at.along_x(k))
        greet(at.along_y(k))
    greet(at.partner)
    pl.when(at.off)(lambda: greet(at.mirror))
    total = 14 + at.off.astype(jnp.int32)
    for when, device in extra:
        pl.when(when)(functools.partial(greet, device))
        total = total + when.astype(jnp.int32)
    return barrier, greet, total


class Spread64:
    def __init__(self, at, copies, buf, src):
        slot = buf.at[at.r, at.zh, at.core]
        self.a = [copies.new(src, slot, at.along_z(k)) for k in range(1, 8)]
        part = buf.at[pl.ds(2 * at.x, 2), :, at.core]
        self.b = [copies.new(part, part, at.along_x(k)) for k in range(1, 4)]
        part = buf.at[:, :, at.core]
        self.d = [copies.new(part, part, at.partner)]

    def first(self):
        start(*self.a)

    def second(self):
        arrive(*self.a)
        start(*self.b)

    def third(self):
        arrive(*self.b)
        start(*self.d)

    def last(self):
        arrive(*self.d)


class Blocks:
    def __init__(self, at, copies, rows, cols, src):
        new = copies.new
        up, down = {"col": 2 * ((at.zh + 1) % 4) + at.core}, {"col": 2 * ((at.zh + 3) % 4) + at.core}
        mine = rows.at[at.c]
        below, above = 2 * ((at.zh + 3) % 4) + at.core, 2 * ((at.zh + 1) % 4) + at.core
        far = 2 * ((at.zh + 2) % 4) + at.core
        self.perm = new(src, cols.at[at.c], at.mirror, at.off)
        self.b = [new(src, mine, up), new(src, mine, down)]
        self.own = new(src, mine, at.partner)
        half = lambda ref, s, h, dev: new(ref.at[s, h], ref.at[s, h], dev)
        self.bfar = [half(rows, below, LOW, up), half(rows, above, HIGH, down)]
        self.fwd = [half(rows, s, WHOLE, at.partner) for s in (below, above)]
        self.fwdfar = half(rows, far, WHOLE, at.partner)
        self.zl = half(cols, at.r, WHOLE, {"row": 2 * at.x + 1 - at.zl})
        self.near, self.relay = [], []
        for zl in (at.zl, 1 - at.zl):
            here, left, right = (2 * ((at.x + k) % 4) + zl for k in (0, 3, 1))
            self.near.append([half(cols, here, WHOLE, at.along_x(k)) for k in (1, 3)])
            self.relay.append([half(cols, left, LOW, at.along_x(1)), half(cols, right, HIGH, at.along_x(3))])

    def first(self):
        start(self.perm, *self.b, self.own)

    def second(self):
        arrive(self.perm)
        start(self.zl, *self.near[0])

    def third(self):
        arrive(self.zl, *self.b, *self.near[0])
        start(*self.near[1], *self.relay[0], *self.bfar, *self.fwd)

    def fourth(self):
        arrive(*self.near[1], *self.bfar)
        start(*self.relay[1], self.fwdfar)

    def last(self):
        arrive(self.own, *self.relay[0], *self.relay[1], *self.fwd, self.fwdfar)


class Scatter16:
    def __init__(self, at, piece, buf, send, recv):
        self.at, self.piece, self.buf, self.send, self.recv = at, piece, buf, send, recv
        self.source = (at.r == 0) & (at.c < 4)
        self.target = at.d > 0
        slot = buf.at[at.r, at.zh, at.core]
        self.incoming = pltpu.make_async_remote_copy(
            src_ref=slot, dst_ref=slot, send_sem=send.at[0], recv_sem=recv.at[0], device_id=at.partner, device_id_type=MESH
        )

    def device(self, i):
        return {"row": 2 * self.at.c + i // 8, "col": i % 8}

    def each(self, f):
        def step(i, _):
            pl.when((self.at.c > 0) | (i > 0))(lambda: f(i))
            return 0

        @pl.when(self.source)
        def _():
            lax.fori_loop(0, 16, step, 0)

    def copy(self, i):
        to = self.device(i)
        return pltpu.make_async_remote_copy(
            src_ref=self.piece(i), dst_ref=self.buf.at[to["row"], to["col"] // 2, to["col"] % 2],
            send_sem=self.send.at[i], recv_sem=self.recv.at[0], device_id=to, device_id_type=MESH,
        )

    def greet(self, greet):
        self.each(lambda i: greet(self.device(i)))
        pl.when(self.target)(lambda: greet({"row": 0, "col": self.at.x}))
        n = jnp.where(self.source, 16 - (self.at.c == 0).astype(jnp.int32), 0)
        return n + self.target.astype(jnp.int32)

    def first(self):
        self.each(lambda i: self.copy(i).start())

    def arrive(self):
        pl.when(self.target)(self.incoming.wait_recv)

    def drain(self):
        self.each(lambda i: self.copy(i).wait_send())


def inputs_kernel(fr, m, m16, anc, inv, mr, mc, g0, own_a, g, send, recv, s16, r16, sa, ra, la, *scr):
    at = Place()
    copies = Copies(send, recv)
    fronts = Spread64(at, copies, g, fr)
    lead = Spread64(at, copies, g0, g0.at[at.r, at.zh, at.core])
    blocks = Blocks(at, copies, mr, mc, m)
    scatter = Scatter16(at, lambda i: m16.at[i], g0, s16, r16)
    here = at.zh == at.l
    left = at.c == 0
    corner = left & (at.l == 0)

    def handed(e):
        rows = pl.ds(pl.multiple_of(256 * at.l + 128 * e, 128), 128)
        return pltpu.make_async_remote_copy(
            src_ref=anc.at[rows, pl.ds(0, 512)], dst_ref=own_a, send_sem=sa.at[e], recv_sem=ra.at[0],
            device_id={"col": 2 * at.l + e}, device_id_type=MESH,
        )

    hand = [(handed(0), left & (at.l > 0)), (handed(1), left)]
    kept = pltpu.make_async_copy(anc.at[pl.ds(0, 128), pl.ds(0, 512)], own_a, la)
    over_y = [
        (pltpu.make_async_remote_copy(
            src_ref=own_a, dst_ref=own_a, send_sem=sa.at[1 + k], recv_sem=ra.at[1],
            device_id=at.along_y(k), device_id_type=MESH,
        ), here)
        for k in range(1, 4)
    ]
    cross = at.core == 1
    extra = [
        (left & (at.l > 0), {"col": 2 * at.l + 1}),
        (here & cross & (at.l > 0), {"col": 0}),
    ]
    barrier, greet, total = meet(at, extra)
    total = total + scatter.greet(greet)
    pl.semaphore_wait(barrier, total)

    fronts.first()
    scatter.first()
    g[at.r, at.zh, at.core] = fr[...]
    mr[at.c] = m[...]

    @pl.when(at.r == at.c)
    def _():
        mc[at.r] = m[...]

    @pl.when(at.d == 0)
    def _():
        g0[0, 0, 0] = m16[0]

    fronts.second()
    blocks.first()
    start(*hand)
    pl.when(corner)(kept.start)
    fronts.third()
    fronts.last()

    def stage0():
        scatter.arrive()
        lead.first()
        blocks.second()

    def stage1():
        lead.second()
        blocks.third()
        pl.when(corner)(kept.wait)
        pl.when(here & jnp.logical_not(corner))(hand[0][0].wait_recv)
        start(*over_y)

    def stage2():
        lead.third()
        blocks.fourth()

    a, y, dt, xr = (scr[i * 2:(i + 1) * 2] for i in range(4))

    def move(r, _):
        for zh in range(4):
            for core in range(2):
                rows = pl.ds(pl.multiple_of(64 * r + 16 * zh + 8 * core, 8), 8)
                for p in range(2):
                    a[p][rows, :] = g[r, zh, core, p].astype(F32)
        return 0

    lax.fori_loop(0, 8, move, 0)
    chol_steps(a, y, dt, xr, [stage0, stage1, stage2])
    for p in range(2):
        inv[p] = y[p][...].astype(BF16)
    blocks.last()
    lead.last()
    pl.when(jnp.logical_not(here))(over_y[0][0].wait_recv)
    for copy, when in over_y + hand:
        pl.when(when)(copy.wait_send)
    copies.drain()
    scatter.drain()


def sems(n):
    return pltpu.SemaphoreType.DMA((n,))


def gather_inputs(fr, m, anc):
    s = jax.ShapeDtypeStruct
    vm = pl.BlockSpec(memory_space=VM)
    return pl.pallas_call(
        inputs_kernel,
        out_shape=[
            s((2, N, N), BF16), s((8, 128, 1024), BF16), s((8, 128, 1024), BF16), s((8, 4, 2, 8, 1024), BF16), s((128, 512), F32),
        ],
        in_specs=[vm, vm, vm, pl.BlockSpec(memory_space=pl.ANY)],
        out_specs=[vm] * 5,
        scratch_shapes=[
            pltpu.VMEM((8, 4, 2, 2, 8, 512), BF16), sems(48), sems(48), sems(16), sems(1), sems(5), sems(2),
            pltpu.SemaphoreType.DMA, *chol_scratch(2),
        ],
        compiler_params=pltpu.CompilerParams(has_side_effects=True, collective_id=1),
    )(fr, m, m.reshape(16, 8, 1024), anc)


def pivot_kernel(q, own_a, pinv, lead, cr, cc, gp, parts, send, recv, s16, r16, a, dt, xr):
    at = Place()
    copies = Copies(send, recv)
    ys = [copies.new(q, parts.at[at.l], at.along_y(k)) for k in range(1, 4)]
    spread = Spread64(at, copies, gp, gp.at[at.r, at.zh, at.core])
    blocks = Blocks(at, copies, cr, cc, lead)
    scatter = Scatter16(at, lambda i: lead.at[pl.ds(pl.multiple_of(8 * i, 8), 8)], gp, s16, r16)
    barrier, greet, total = meet(at)
    total = total + scatter.greet(greet)
    pl.semaphore_wait(barrier, total)
    start(*ys)
    parts[at.l] = q[...]
    arrive(*ys)
    terms = [parts[i].astype(F32) for i in range(4)]
    lead[...] = own_a[...] - (((terms[0] + terms[1]) + terms[2]) + terms[3])
    scatter.first()
    cr[at.c] = lead[...]

    @pl.when(at.r == at.c)
    def _():
        cc[at.r] = lead[...]

    @pl.when(at.d == 0)
    def _():
        gp[0, 0, 0] = lead[0:8, :]

    scatter.arrive()
    spread.first()
    spread.second()
    blocks.first()
    spread.third()
    spread.last()

    def move(r, _):
        for zh in range(4):
            for core in range(2):
                a[pl.ds(pl.multiple_of(64 * r + 16 * zh + 8 * core, 8), 8), :] = gp[r, zh, core]
        return 0

    lax.fori_loop(0, 8, move, 0)
    chol_steps([a], [pinv], [dt], [xr], [blocks.second, blocks.third, blocks.fourth])
    blocks.last()
    copies.drain()
    scatter.drain()


def gather_pivot(q, own_a):
    s = jax.ShapeDtypeStruct
    vm = pl.BlockSpec(memory_space=VM)
    return pl.pallas_call(
        pivot_kernel,
        out_shape=[s((N, N), F32), s((128, 512), F32), s((8, 128, 512), F32), s((8, 128, 512), F32)],
        in_specs=[vm, vm],
        out_specs=[vm] * 4,
        scratch_shapes=[
            pltpu.VMEM((8, 4, 2, 8, 512), F32), pltpu.VMEM((4, 128, 512), BF16), sems(40), sems(40), sems(16), sems(1),
            *chol_scratch(1, False),
        ],
        compiler_params=pltpu.CompilerParams(has_side_effects=True, collective_id=2),
        cost_estimate=pl.CostEstimate(flops=4_000_000_000, bytes_accessed=8_000_000, transcendentals=0),
    )(q, own_a)


def local(ancestor, coupling, fronts, tile_pattern):
    r, c = lax.axis_index("row"), lax.axis_index("col")
    fr = jnp.swapaxes(fronts[0], 1, 2).astype(BF16)
    on = lax.dynamic_slice_in_dim(tile_pattern[0], r, 1, 1)
    masked = coupling[0] * jnp.repeat(on[:, 0], 512)[None, :].astype(BF16)
    inv, mr, mc, m0, own_a = gather_inputs(fr, masked, ancestor)

    def solved(rows):
        out = [
            lax.dot_general(rows[:, p * 512:(p + 1) * 512], inv[p], (((1,), (1,)), ((), ())), preferred_element_type=F32)
            for p in range(2)
        ]
        return jnp.concatenate(out, 1).astype(BF16)

    outer = lambda a, b: lax.dot_general(a, b, (((1,), (1,)), ((), ())), preferred_element_type=F32)
    q = outer(solved(masked), solved(m0.reshape(512, 1024))).astype(BF16)
    row_side, col_side = solved(mr.reshape(1024, 1024)), solved(mc.reshape(1024, 1024))
    update = outer(row_side, col_side).astype(BF16)
    q, update = lax.optimization_barrier((q, update))
    summed = lax.psum(update, "layer")
    pinv, lead, cr, cc = gather_pivot(q, own_a)
    high = functools.partial(
        lax.dot_general, dimension_numbers=(((1,), (1,)), ((), ())), precision=lax.Precision.HIGH, preferred_element_type=F32
    )
    rows = high(cr.reshape(1024, 512), pinv)
    cols = high(cc.reshape(1024, 512), pinv)
    schur = ancestor - summed.astype(F32) - high(rows, cols)
    panel = high(lead, pinv)
    scale = jnp.diagonal(lax.dynamic_slice(pinv, (8 * (8 * r + c), 0), (8, 512)).reshape(8, 64, 8)[:, 8 * r + c])
    return schur, panel, 1.0 / (scale * scale)


def solution(mesh):
    return jax.shard_map(
        local,
        mesh=mesh,
        in_specs=(
            P("row", "col"),
            P("layer", ("row", "col"), None),
            P("layer", None, None, ("row", "col")),
            P("layer", None, None),
        ),
        out_specs=(P("row", "col"), P(("row", "col"), None), P(("row", "col"))),
        check_vma=False,
    )
```
